32 devices in a mesh: dp: 1 (over z), tp: 32 (over x, y, core).
Axes of the slice: x: 4, y: 4, z: 1, core: 2. Of those that a mesh axis runs over, the one named last changes fastest.
The devices are a block of a 4x4x8 slice.
Arguments:
- x: bfloat16 [2048, 2048], P('dp')
- dy: bfloat16 [2048, 2048], P('dp')
- gate: bfloat16 [2048, 16384], P('dp', 'tp')
- up: bfloat16 [2048, 16384], P('dp', 'tp')
- w_gate: bfloat16 [2048, 16384], P(None, 'tp')
- w_up: bfloat16 [2048, 16384], P(None, 'tp')
- w_down: bfloat16 [16384, 2048], P('tp')
Outputs:
- output 1: bfloat16 [2048, 2048], P('dp')
- output 2: bfloat16 [2048, 16384], P('dp', 'tp')
- output 3: bfloat16 [2048, 16384], P('dp', 'tp')
- output 4: bfloat16 [16384, 2048], P(('dp', 'tp'))
All inputs are finite; a program needn't handle non-finite values.
Results may differ from the reference program's by a relative error of at most 0.012.
Values are sent between devices in bfloat16 or wider.
A program may use at most 768 MiB of HBM per device.

```python
import jax
import jax.numpy as jnp

ROWS = 2048
D = 2048
FF = 16384


def act(gate, up):
    return jax.nn.gelu(gate) * up


def setup_inputs(seed: int = 0, part: int = 0) -> dict:
    kx, ky, ka, kb, kg, ku, kd = jax.random.split(jax.random.key(seed), 7)
    kx, ky, ka, kb = (jax.random.fold_in(k, part) for k in (kx, ky, ka, kb))
    drawn = {
        "x": jax.random.normal(kx, (ROWS, D), jnp.float32),
        "dy": jax.random.normal(ky, (ROWS, D), jnp.float32),
        "gate": jax.random.normal(ka, (ROWS, FF), jnp.float32),
        "up": jax.random.normal(kb, (ROWS, FF), jnp.float32),
        "w_gate": jax.random.normal(kg, (D, FF), jnp.float32) * D**-0.5,
        "w_up": jax.random.normal(ku, (D, FF), jnp.float32) * D**-0.5,
        "w_down": jax.random.normal(kd, (FF, D), jnp.float32) * FF**-0.5,
    }
    return {k: v.astype(jnp.bfloat16) for k, v in drawn.items()}


def reference(x, dy, gate, up, w_gate, w_up, w_down):
    hidden, back = jax.vjp(act, gate.astype(jnp.float32), up.astype(jnp.float32))
    d_hidden = jnp.dot(dy, w_down.T, preferred_element_type=jnp.float32)
    d_gate, d_up = (g.astype(jnp.bfloat16) for g in back(d_hidden))
    dx = jnp.dot(d_gate, w_gate.T, preferred_element_type=jnp.float32) + jnp.dot(d_up, w_up.T, preferred_element_type=jnp.float32)
    dw_gate = jnp.dot(x.T, d_gate, preferred_element_type=jnp.float32)
    dw_up = jnp.dot(x.T, d_up, preferred_element_type=jnp.float32)
    dw_down = jnp.dot(hidden.astype(jnp.bfloat16).T, dy, preferred_element_type=jnp.float32)
    return tuple(g.astype(jnp.bfloat16) for g in (dx, dw_gate, dw_up, dw_down))
```

```python
import functools
import math

import jax
import jax.numpy as jnp
from jax import lax
from jax.experimental import pallas as pl
from jax.experimental.pallas import tpu as pltpu
from jax.sharding import PartitionSpec as P

MESH = pl.DeviceIdType.MESH
CHUNK = 256
BF16, F32 = jnp.bfloat16, jnp.float32
COPIES = 21
SLOTS = 5


def dot(a, b, ca, cb):
    return lax.dot_general(a, b, (((ca,), (cb,)), ((), ())), preferred_element_type=F32)


def kernel(side, x, dy, gate, up, wg, wu, wd, dx, dwg, dwu, dwd,
           wdv, wv, dyv, gu, hid, xs, own, sT, rT, sA, rA, sB, rB, sC, rC, sD, rD, wsem, lsem, xsem, ssem, rsem):
    rows, d = dx.shape
    f = wd.shape[0]
    m = min(CHUNK, rows)
    n = rows // m
    half, q = m // 2, m // 8
    ch, cq, ce = d // 2, d // 4, d // 8
    units, uw = n, d // n

    me = lax.axis_index("tp")
    core = lax.rem(me, 2)
    chip = me // 2
    px, py = chip // side, lax.rem(chip, side)
    p1 = px + core * (py - px)
    p2 = py + core * (px - py)

    def at(a, b):
        return ((1 - core) * (a * side + b) + core * (b * side + a)) * 2 + core

    def turn(p, k):
        return lax.rem(p + k, side)

    r1, o1, l1 = turn(p1, 1), turn(p1, 2), turn(p1, 3)
    r2, o2, l2 = turn(p2, 1), turn(p2, 2), turn(p2, 3)
    partner = me + 1 - 2 * core
    first = (at(r1, p2), at(l1, p2))
    second = (at(p1, r2), at(p1, l2))

    barrier = pltpu.get_barrier_semaphore()
    for dev in (partner, *first, *second):
        pl.semaphore_signal(barrier, inc=1, device_id={"tp": dev}, device_id_type=MESH)

    def load(src, dst, sem):
        return pltpu.make_async_copy(src, dst, sem)

    def chunk_loads(c):
        r = pl.ds(pl.multiple_of(c * m, m), m)
        return (
            load(dy.at[r], dyv.at[r], lsem.at[c, 0]),
            load(gate.at[r], gu.at[r, pl.ds(0, f)], lsem.at[c, 1]),
            load(up.at[r], gu.at[r, pl.ds(f, f)], lsem.at[c, 2]),
        )

    def unit_load(j, slot):
        return load(x.at[:, pl.ds(pl.multiple_of(j * uw, uw), uw)], xs.at[slot], xsem.at[slot])

    load_wd = load(wd, wdv, wsem.at[0])
    load_wg = load(wg, wv.at[:, pl.ds(0, f)], wsem.at[1])
    load_wu = load(wu, wv.at[:, pl.ds(f, f)], wsem.at[2])
    load_wd.start()
    for cp in chunk_loads(0):
        cp.start()
    load_wg.start()
    load_wu.start()
    for c in range(1, min(3, n)):
        for cp in chunk_loads(c):
            cp.start()
    pl.semaphore_wait(barrier, 5)

    def send(c, k, src, dst, dev):
        return pltpu.make_async_remote_copy(
            src, dst, ssem.at[c, k], rsem.at[c, k], device_id={"tp": dev}, device_id_type=MESH
        )

    def place(c, h, piece):
        return pl.ds(pl.multiple_of(c * m + h * half + piece * q, q), q)

    def piece(p):
        return pl.ds(pl.multiple_of(p * q, q), q)

    def cols(p, width):
        return pl.ds(pl.multiple_of(p * width, width), width)

    lo, hi, al = pl.ds(0, ch), pl.ds(ch, ch), pl.ds(0, d)

    def same(c, k, r, w, dev):
        return send(c, k, dx.at[r, w], dx.at[r, w], dev)

    def copy(c, k):
        if k == 0:
            return send(c, 0, sT.at[c], rT.at[c], partner)
        if k <= 2:
            return send(c, k, sA.at[c, k - 1], rA.at[c, k - 1], first[k - 1])
        if k <= 4:
            return send(c, k, sB.at[c, k - 3], rB.at[c, k - 3], first[k - 3])
        if k <= 6:
            return send(c, k, sC.at[c, k - 5], rC.at[c, k - 5], second[k - 5])
        if k <= 8:
            return send(c, k, sD.at[c, k - 7], rD.at[c, k - 7], second[k - 7])
        mine = place(c, core, p1)
        if k <= 10:
            return same(c, k, mine, cols(p2, cq), second[k - 9])
        if k == 11:
            return same(c, k, mine, cols(2 * l2, ce), second[0])
        if k == 12:
            return same(c, k, mine, cols(2 * r2 + 1, ce), second[1])
        if k <= 14:
            return same(c, k, mine, al, first[k - 13])
        if k == 15:
            return same(c, k, place(c, core, l1), lo, first[0])
        if k == 16:
            return same(c, k, place(c, core, r1), hi, first[1])
        return same(c, k, place(c, core, (p1, l1, r1, o1)[k - 17]), al, partner)

    def arrival(c, k):
        if k <= 8:
            return copy(c, k)
        mine = place(c, core, p1)
        if k <= 10:
            return same(c, k, mine, cols((l2, r2)[k - 9], cq), partner)
        if k <= 12:
            return same(c, k, mine, cols(2 * o2 + (k - 11), ce), partner)
        if k <= 14:
            return same(c, k, place(c, core, (l1, r1)[k - 13]), al, partner)
        if k <= 16:
            return same(c, k, place(c, core, o1), (lo, hi)[k - 15], partner)
        s = (p2, l2, r2, o2)[k - 17]
        return same(c, k, place(c, 1 - core, s), al, partner)

    def got(c, *ks):
        for k in ks:
            arrival(c, k).wait_recv()

    def go(c, *ks):
        for k in ks:
            copy(c, k).start()

    def event(k, c):
        acc = own.at[lax.rem(c, SLOTS)]
        if k == 1:
            got(c, 0)
            t = acc[piece(o1), :] + rT[c, piece(o1), :].astype(F32)
            sA[c, 0] = t[:, :ch].astype(BF16)
            sA[c, 1] = t[:, ch:].astype(BF16)
            for p in (r1, l1, p1):
                acc[piece(p), :] = acc[piece(p), :] + rT[c, piece(p), :].astype(F32)
            go(c, 1, 2)
        elif k == 2:
            got(c, 1, 2)
            sB[c, 0, :, lo] = (acc[piece(r1), lo] + rA[c, 0].astype(F32)).astype(BF16)
            sB[c, 0, :, hi] = acc[piece(r1), hi].astype(BF16)
            sB[c, 1, :, lo] = acc[piece(l1), lo].astype(BF16)
            sB[c, 1, :, hi] = (acc[piece(l1), hi] + rA[c, 1].astype(F32)).astype(BF16)
            go(c, 3, 4)
        elif k == 3:
            got(c, 3, 4)
            acc[piece(p1), :] = acc[piece(p1), :] + rB[c, 0].astype(F32) + rB[c, 1].astype(F32)
            sC[c, 0] = acc[piece(p1), cols(2 * o2, ce)].astype(BF16)
            sC[c, 1] = acc[piece(p1), cols(2 * o2 + 1, ce)].astype(BF16)
            go(c, 5, 6)
        elif k == 4:
            got(c, 5, 6)
            sD[c, 0, :, :ce] = (acc[piece(p1), cols(2 * r2, ce)] + rC[c, 0].astype(F32)).astype(BF16)
            sD[c, 0, :, ce:] = acc[piece(p1), cols(2 * r2 + 1, ce)].astype(BF16)
            sD[c, 1, :, :ce] = acc[piece(p1), cols(2 * l2, ce)].astype(BF16)
            sD[c, 1, :, ce:] = (acc[piece(p1), cols(2 * l2 + 1, ce)] + rC[c, 1].astype(F32)).astype(BF16)
            go(c, 7, 8)
        elif k == 5:
            got(c, 7, 8)
            t = acc[piece(p1), cols(p2, cq)] + rD[c, 0].astype(F32) + rD[c, 1].astype(F32)
            dx[place(c, core, p1), cols(p2, cq)] = t.astype(BF16)
            go(c, 9, 10)
        elif k == 6:
            got(c, 9, 10)
            go(c, 11, 12)
        elif k == 7:
            got(c, 11, 12)
            go(c, 13, 14, 17)
        elif k == 8:
            got(c, 13, 14)
            go(c, 15, 16, 18, 19)
        elif k == 9:
            got(c, 15, 16)
            go(c, 20)
        else:
            got(c, 17, 18, 19, 20)

    c0, c1 = math.sqrt(2 / math.pi), math.sqrt(2 / math.pi) * 0.044715

    def hidden_part(c):
        for cp in chunk_loads(c):
            cp.wait()
        r = pl.ds(pl.multiple_of(c * m, m), m)
        for lo_f in range(0, f, f // 2):
            w = pl.ds(lo_f, f // 2)
            w2 = pl.ds(f + lo_f, f // 2)
            dh = dot(dyv[r, :], wdv[w, :], 1, 1)
            g = gu[r, w].astype(F32)
            u = gu[r, w2].astype(F32)
            g2 = g * g
            t = jnp.tanh(g * (c0 + c1 * g2))
            hg = 0.5 * g
            s = 1.0 + t
            act = hg * s
            slope = 0.5 * s + hg * (s * (1.0 - t)) * (c0 + (3.0 * c1) * g2)
            hid[r, w] = (act * u).astype(BF16)
            gu[r, w] = (dh * u * slope).astype(BF16)
            gu[r, w2] = (dh * act).astype(BF16)

    def term_part(c):
        base = c * m
        rp = pl.ds(pl.multiple_of(base + (1 - core) * half, half), half)
        ro = pl.ds(pl.multiple_of(base + core * half, half), half)
        acc = own.at[lax.rem(c, SLOTS)]
        lhs = jnp.concatenate([gu[rp, :], gu[ro, :]], 0)
        for k in range(4):
            w = pl.ds(k * cq, cq)
            t = dot(lhs, wv[w, :], 1, 1)
            sT[c, :, w] = t[:half].astype(BF16)
            acc[:, w] = t[half:]
        go(c, 0)

    def weights_part(j):
        unit_load(j, lax.rem(j, 2)).wait()
        r = pl.ds(pl.multiple_of(j * uw, uw), uw)
        t = dot(xs[lax.rem(j, 2)], gu[...], 0, 0)
        dwg[r, :] = t[:, :f].astype(BF16)
        dwu[r, :] = t[:, f:].astype(BF16)

    def down_part(j):
        w = pl.ds(pl.multiple_of(j * uw, uw), uw)
        dwd[:, w] = dot(hid[...], dyv[:, w], 0, 0).astype(BF16)

    load_wd.wait()

    def step(t, _):
        @pl.when(t < n)
        def _():
            hidden_part(t)

        j = t - n

        @pl.when((j >= 0) & (j < units))
        def _():
            weights_part(j)

            @pl.when(j + 2 < units)
            def _():
                unit_load(j + 2, lax.rem(j, 2)).start()

        for k in range(1, 11):
            @pl.when((t - k >= 0) & (t - k < n))
            def _(k=k):
                event(k, t - k)

        @pl.when(t == 0)
        def _():
            load_wg.wait()
            load_wu.wait()

        @pl.when(t < n)
        def _():
            term_part(t)

            @pl.when(t + 3 < n)
            def _():
                for cp in chunk_loads(t + 3):
                    cp.start()

        @pl.when(t == n - 3)
        def _():
            unit_load(0, 0).start()
            unit_load(1, 1).start()

        @pl.when((j >= 0) & (j < units))
        def _():
            down_part(j)

        return 0

    lax.fori_loop(0, n + 10, step, 0)

    def drain(c, _):
        for k in range(COPIES):
            copy(c, k).wait_send()
        return 0

    lax.fori_loop(0, n, drain, 0)


def solution(mesh):
    side = math.isqrt(mesh.shape["tp"] // 2)

    def step(x, dy, gate, up, w_gate, w_up, w_down):
        (rows, d), f = x.shape, gate.shape[1]
        m = min(CHUNK, rows)
        n, half, q = rows // m, m // 2, m // 8
        vm = pltpu.VMEM
        return tuple(pl.pallas_call(
            functools.partial(kernel, side),
            out_shape=[vm((rows, d), BF16), vm((d, f), BF16), vm((d, f), BF16), vm((f, d), BF16)],
            in_specs=[pl.BlockSpec(memory_space=pl.ANY)] * 7,
            out_specs=[pl.BlockSpec(memory_space=pltpu.VMEM)] * 4,
            scratch_shapes=[
                vm((f, d), BF16), vm((d, 2 * f), BF16), vm((rows, d), BF16), vm((rows, 2 * f), BF16), vm((rows, f), BF16),
                vm((2, rows, d // n), BF16), vm((SLOTS, half, d), F32),
                vm((n, half, d), BF16), vm((n, half, d), BF16),
                vm((n, 2, q, d // 2), BF16), vm((n, 2, q, d // 2), BF16),
                vm((n, 2, q, d), BF16), vm((n, 2, q, d), BF16),
                vm((n, 2, q, d // 8), BF16), vm((n, 2, q, d // 8), BF16),
                vm((n, 2, q, d // 4), BF16), vm((n, 2, q, d // 4), BF16),
                pltpu.SemaphoreType.DMA((3,)), pltpu.SemaphoreType.DMA((n, 3)), pltpu.SemaphoreType.DMA((2,)),
                pltpu.SemaphoreType.DMA((n, COPIES)), pltpu.SemaphoreType.DMA((n, COPIES)),
            ],
            compiler_params=pltpu.CompilerParams(
                collective_id=0, has_side_effects=True, vmem_limit_bytes=49 * 2**20
            ),
        )(x, dy, gate, up, w_gate, w_up, w_down))

    tokens, columns, by_rows = P("dp", None), P(None, "tp"), P("tp", None)
    return jax.shard_map(
        step,
        mesh=mesh,
        in_specs=(tokens, tokens, P("dp", "tp"), P("dp", "tp"), columns, columns, by_rows),
        out_specs=(tokens, P("dp", "tp"), P("dp", "tp"), P(("dp", "tp"), None)),
        check_vma=False,
    )
```

```python
import functools
import math

import jax
import jax.numpy as jnp
from jax import lax
from jax.experimental import pallas as pl
from jax.experimental.pallas import tpu as pltpu
from jax.sharding import PartitionSpec as P

MESH = pl.DeviceIdType.MESH
CHUNK = 256
BF16, F32 = jnp.bfloat16, jnp.float32
COPIES = 19
SLOTS = 6
POINTS = 3
LAG = {1: 4, 2: 9, 3: 14, 4: 20, 5: 28, 6: 43, 7: 75, 8: 81}


def dot(a, b, ca, cb):
    return lax.dot_general(a, b, (((ca,), (cb,)), ((), ())), preferred_element_type=F32)


def kernel(side, x, dy, gate, up, wg, wu, wd, dx, dwg, dwu, dwd,
           wdv, wv, dyv, gu, hid, xs, own, fin, sT, rT, sA, rA, sB, rB, sC, rC, wsem, lsem, xsem, ssem, rsem):
    rows, d = dx.shape
    f = wd.shape[0]
    m = min(CHUNK, rows)
    n = rows // m
    half, q = m // 2, m // 8
    ch, cq = d // 2, d // 4
    units, uw = n, d // n

    me = lax.axis_index("tp")
    core = lax.rem(me, 2)
    chip = me // 2
    px, py = chip // side, lax.rem(chip, side)
    p1 = px + core * (py - px)
    p2 = py + core * (px - py)

    def at(a, b):
        return ((1 - core) * (a * side + b) + core * (b * side + a)) * 2 + core

    def turn(p, k):
        return lax.rem(p + k, side)

    r1, o1, l1 = turn(p1, 1), turn(p1, 2), turn(p1, 3)
    r2, o2, l2 = turn(p2, 1), turn(p2, 2), turn(p2, 3)
    partner = me + 1 - 2 * core
    first = (at(r1, p2), at(l1, p2))
    second = (at(p1, r2), at(p1, l2), at(p1, o2))

    barrier = pltpu.get_barrier_semaphore()
    for dev in (partner, *first, *second):
        pl.semaphore_signal(barrier, inc=1, device_id={"tp": dev}, device_id_type=MESH)

    def load(src, dst, sem):
        return pltpu.make_async_copy(src, dst, sem)

    def chunk_loads(c):
        r = pl.ds(pl.multiple_of(c * m, m), m)
        return (
            load(dy.at[r], dyv.at[r], lsem.at[c, 0]),
            load(gate.at[r], gu.at[r, pl.ds(0, f)], lsem.at[c, 1]),
            load(up.at[r], gu.at[r, pl.ds(f, f)], lsem.at[c, 2]),
        )

    def unit_load(j, slot):
        return load(x.at[:, pl.ds(pl.multiple_of(j * uw, uw), uw)], xs.at[slot], xsem.at[slot])

    load_wd = load(wd, wdv, wsem.at[0])
    load_wg = load(wg, wv.at[:, pl.ds(0, f)], wsem.at[1])
    load_wu = load(wu, wv.at[:, pl.ds(f, f)], wsem.at[2])
    first_loads = chunk_loads(0)
    for cp in (first_loads[1], first_loads[2], first_loads[0], load_wd):
        cp.start()

    def send(c, k, src, dst, dev):
        return pltpu.make_async_remote_copy(
            src, dst, ssem.at[c, k], rsem.at[c, k], device_id={"tp": dev}, device_id_type=MESH
        )

    def place(c, h, piece):
        return pl.ds(pl.multiple_of(c * m + h * half + piece * q, q), q)

    def piece(p):
        return pl.ds(pl.multiple_of(p * q, q), q)

    def cols(p, width):
        return pl.ds(pl.multiple_of(p * width, width), width)

    lo, hi, al = pl.ds(0, ch), pl.ds(ch, ch), pl.ds(0, d)

    def same(c, k, r, w, dev):
        return send(c, k, dx.at[r, w], dx.at[r, w], dev)

    def copy(c, k):
        if k == 0:
            return send(c, 0, sT.at[c], rT.at[c], partner)
        if k <= 2:
            return send(c, k, sA.at[c, k - 1], rA.at[c, k - 1], first[k - 1])
        if k <= 4:
            return send(c, k, sB.at[c, k - 3], rB.at[c, k - 3], first[k - 3])
        if k <= 7:
            return send(c, k, sC.at[c, k - 5], rC.at[c, k - 5], second[k - 5])
        mine = place(c, core, p1)
        if k <= 10:
            return same(c, k, mine, cols(p2, cq), second[k - 8])
        if k <= 12:
            return same(c, k, mine, al, first[k - 11])
        if k == 13:
            return same(c, k, place(c, core, l1), lo, first[0])
        if k == 14:
            return same(c, k, place(c, core, r1), hi, first[1])
        return same(c, k, place(c, core, (p1, l1, r1, o1)[k - 15]), al, partner)

    def arrival(c, k):
        if k <= 7:
            return copy(c, k)
        mine = place(c, core, p1)
        if k <= 10:
            return same(c, k, mine, cols((l2, r2, o2)[k - 8], cq), partner)
        if k <= 12:
            return same(c, k, place(c, core, (l1, r1)[k - 11]), al, partner)
        if k <= 14:
            return same(c, k, place(c, core, o1), (lo, hi)[k - 13], partner)
        s = (p2, l2, r2, o2)[k - 15]
        return same(c, k, place(c, 1 - core, s), al, partner)

    def got(c, *ks):
        for k in ks:
            arrival(c, k).wait_recv()

    def go(c, *ks):
        for k in ks:
            copy(c, k).start()

    def event(k, c):
        acc = own.at[lax.rem(c, SLOTS)]
        if k == 1:
            got(c, 0)
            t = acc[piece(o1), :] + rT[c, piece(o1), :].astype(F32)
            sA[c, 0] = t[:, :ch].astype(BF16)
            sA[c, 1] = t[:, ch:].astype(BF16)
            for p in (r1, l1, p1):
                acc[piece(p), :] = acc[piece(p), :] + rT[c, piece(p), :].astype(F32)
            go(c, 1, 2)
        elif k == 2:
            got(c, 1, 2)
            sB[c, 0, :, lo] = (acc[piece(r1), lo] + rA[c, 0].astype(F32)).astype(BF16)
            sB[c, 0, :, hi] = acc[piece(r1), hi].astype(BF16)
            sB[c, 1, :, lo] = acc[piece(l1), lo].astype(BF16)
            sB[c, 1, :, hi] = (acc[piece(l1), hi] + rA[c, 1].astype(F32)).astype(BF16)
            go(c, 3, 4)
        elif k == 3:
            got(c, 3, 4)
            acc[piece(p1), :] = acc[piece(p1), :] + rB[c, 0].astype(F32) + rB[c, 1].astype(F32)
            for i, p in enumerate((r2, l2, o2)):
                sC[c, i] = acc[piece(p1), cols(p, cq)].astype(BF16)
            fin[c] = acc[piece(p1), cols(p2, cq)]
            go(c, 5, 6, 7)
        elif k == 4:
            got(c, 5, 6, 7)
            t = fin[c] + rC[c, 0].astype(F32) + rC[c, 1].astype(F32) + rC[c, 2].astype(F32)
            dx[place(c, core, p1), cols(p2, cq)] = t.astype(BF16)
            go(c, 8, 9, 10)
        elif k == 5:
            got(c, 8, 9, 10)
            go(c, 11, 12, 15)
        elif k == 6:
            got(c, 11, 12)
            go(c, 13, 14, 16, 17)
        elif k == 7:
            got(c, 13, 14)
            go(c, 18)
        else:
            got(c, 15, 16, 17, 18)

    c0, c1 = math.sqrt(2 / math.pi), math.sqrt(2 / math.pi) * 0.044715

    def hidden_part(c):
        r = pl.ds(pl.multiple_of(c * m, m), m)
        w, w2 = pl.ds(0, f), pl.ds(f, f)
        dh = dot(dyv[r, :], wdv[w, :], 1, 1)
        g = gu[r, w].astype(F32)
        u = gu[r, w2].astype(F32)
        g2 = g * g
        t = jnp.tanh(g * (c0 + c1 * g2))
        hg = 0.5 * g
        s = 1.0 + t
        act = hg * s
        slope = 0.5 * s + hg * (s * (1.0 - t)) * (c0 + (3.0 * c1) * g2)
        hid[r, w] = (act * u).astype(BF16)
        gu[r, w] = (dh * u * slope).astype(BF16)
        gu[r, w2] = (dh * act).astype(BF16)

    def term_part(c, k):
        base = c * m
        rp = pl.ds(pl.multiple_of(base + (1 - core) * half, half), half)
        ro = pl.ds(pl.multiple_of(base + core * half, half), half)
        w = pl.ds(k * ch, ch)
        t = dot(jnp.concatenate([gu[rp, :], gu[ro, :]], 0), wv[w, :], 1, 1)
        sT[c, :, w] = t[:half].astype(BF16)
        own[lax.rem(c, SLOTS), :, w] = t[half:]

    def weights_part(j):
        r = pl.ds(pl.multiple_of(j * uw, uw), uw)
        t = dot(xs[lax.rem(j, 2)], gu[...], 0, 0)
        dwg[r, :] = t[:, :f].astype(BF16)
        dwu[r, :] = t[:, f:].astype(BF16)

    def down_part(j):
        w = pl.ds(pl.multiple_of(j * uw, uw), uw)
        dwd[:, w] = dot(hid[...], dyv[:, w], 0, 0).astype(BF16)

    def dx_piece(c, i):
        if i == 0:
            for cp in chunk_loads(c):
                cp.wait()
            hidden_part(c)
        else:
            term_part(c, i - 1)
        if i == 2:
            go(c, 0)

            @pl.when(c + 3 < n)
            def _():
                for cp in chunk_loads(c + 3):
                    cp.start()

            @pl.when(c == n - 3)
            def _():
                unit_load(0, 0).start()
                unit_load(1, 1).start()

    def dw_piece(j, i):
        if i == 0:
            unit_load(j, lax.rem(j, 2)).wait()
            weights_part(j)

            @pl.when(j + 2 < units)
            def _():
                unit_load(j + 2, lax.rem(j, 2)).start()
        elif i == 2:
            down_part(j)

    first_loads[1].wait()
    load_wg.start()
    load_wu.start()
    first_loads[2].wait()
    first_loads[0].wait()
    load_wd.wait()
    hidden_part(0)
    for c in range(1, min(4, n)):
        for cp in chunk_loads(c):
            cp.start()
    load_wg.wait()
    load_wu.wait()
    term_part(0, 0)
    term_part(0, 1)
    pl.semaphore_wait(barrier, 6)
    go(0, 0)

    def step(t, _):
        for i in range(POINTS):
            @pl.when(t < n)
            def _(i=i):
                dx_piece(t, i)

            if i != 1:
                @pl.when((t >= n) & (t < n + units))
                def _(i=i):
                    dw_piece(t - n, i)

            for k, lag in LAG.items():
                if lag % POINTS == i:
                    c = t - lag // POINTS

                    @pl.when((c >= 0) & (c < n))
                    def _(k=k, c=c):
                        event(k, c)

        return 0

    lax.fori_loop(1, n + max(LAG.values()) // POINTS, step, 0)

    def drain(c, _):
        for k in range(COPIES):
            copy(c, k).wait_send()
        return 0

    lax.fori_loop(0, n, drain, 0)


def flush(*refs):
    src, dst, sem = refs[:4], refs[4:8], refs[8]
    copies, cuts = [], (8, 2, 2, 2)
    for a, b, cut in zip(src, dst, cuts):
        size = a.shape[0] // cut
        for i in range(cut):
            r = pl.ds(i * size, size)
            copies.append(pltpu.make_async_copy(a.at[r], b.at[r], sem.at[len(copies)]))
    for cp in copies:
        cp.start()
    for cp in copies:
        cp.wait()


def solution(mesh):
    side = math.isqrt(mesh.shape["tp"] // 2)

    def step(x, dy, gate, up, w_gate, w_up, w_down):
        (rows, d), f = x.shape, gate.shape[1]
        m = min(CHUNK, rows)
        n, half, q = rows // m, m // 2, m // 8
        vm = pltpu.VMEM
        results = pl.pallas_call(
            functools.partial(kernel, side),
            out_shape=[vm((rows, d), BF16), vm((d, f), BF16), vm((d, f), BF16), vm((f, d), BF16)],
            in_specs=[pl.BlockSpec(memory_space=pl.ANY)] * 7,
            out_specs=[pl.BlockSpec(memory_space=pltpu.VMEM)] * 4,
            scratch_shapes=[
                vm((f, d), BF16), vm((d, 2 * f), BF16), vm((rows, d), BF16), vm((rows, 2 * f), BF16), vm((rows, f), BF16),
                vm((2, rows, d // n), BF16), vm((SLOTS, half, d), F32), vm((n, q, d // 4), F32),
                vm((n, half, d), BF16), vm((n, half, d), BF16),
                vm((n, 2, q, d // 2), BF16), vm((n, 2, q, d // 2), BF16),
                vm((n, 2, q, d), BF16), vm((n, 2, q, d), BF16),
                vm((n, 3, q, d // 4), BF16), vm((n, 3, q, d // 4), BF16),
                pltpu.SemaphoreType.DMA((3,)), pltpu.SemaphoreType.DMA((n, 3)), pltpu.SemaphoreType.DMA((2,)),
                pltpu.SemaphoreType.DMA((n, COPIES)), pltpu.SemaphoreType.DMA((n, COPIES)),
            ],
            compiler_params=pltpu.CompilerParams(
                collective_id=0, has_side_effects=True, vmem_limit_bytes=49 * 2**20 + 2**19
            ),
        )(x, dy, gate, up, w_gate, w_up, w_down)
        return tuple(pl.pallas_call(
            flush,
            out_shape=[jax.ShapeDtypeStruct(a.shape, a.dtype) for a in results],
            in_specs=[pl.BlockSpec(memory_space=pltpu.VMEM)] * 4,
            out_specs=[pl.BlockSpec(memory_space=pl.ANY)] * 4,
            scratch_shapes=[pltpu.SemaphoreType.DMA((14,))],
            compiler_params=pltpu.CompilerParams(vmem_limit_bytes=2**20),
        )(*results))

    tokens, columns, by_rows = P("dp", None), P(None, "tp"), P("tp", None)
    return jax.shard_map(
        step,
        mesh=mesh,
        in_specs=(tokens, tokens, P("dp", "tp"), P("dp", "tp"), columns, columns, by_rows),
        out_specs=(tokens, P("dp", "tp"), P("dp", "tp"), P(("dp", "tp"), None)),
        check_vma=False,
    )
```

```python
import functools
import math

import jax
import jax.numpy as jnp
from jax import lax
from jax.experimental import pallas as pl
from jax.experimental.pallas import tpu as pltpu
from jax.sharding import PartitionSpec as P

MESH = pl.DeviceIdType.MESH
CHUNK = 256
BF16, F32 = jnp.bfloat16, jnp.float32
COPIES = 19
SLOTS = 6
POINTS = 2
LAG = {1: 3, 2: 7, 3: 12, 4: 17, 5: 22, 6: 35, 7: 52, 8: 58}


def dot(a, b, ca, cb):
    return lax.dot_general(a, b, (((ca,), (cb,)), ((), ())), preferred_element_type=F32)


def kernel(side, x, dy, gate, up, wg, wu, wd, dx, dwg, dwu, dwd,
           wdv, wv, dyv, gu, hid, xs, own, fin, sT, rT, sA, rA, sB, rB, sC, rC, wsem, lsem, xsem, ssem, rsem):
    rows, d = dx.shape
    f = wd.shape[0]
    m = min(CHUNK, rows)
    n = rows // m
    half, q = m // 2, m // 8
    ch, cq = d // 2, d // 4
    units, uw = n, d // n

    me = lax.axis_index("tp")
    core = lax.rem(me, 2)
    chip = me // 2
    px, py = chip // side, lax.rem(chip, side)
    p1 = px + core * (py - px)
    p2 = py + core * (px - py)

    def at(a, b):
        return ((1 - core) * (a * side + b) + core * (b * side + a)) * 2 + core

    def turn(p, k):
        return lax.rem(p + k, side)

    r1, o1, l1 = turn(p1, 1), turn(p1, 2), turn(p1, 3)
    r2, o2, l2 = turn(p2, 1), turn(p2, 2), turn(p2, 3)
    partner = me + 1 - 2 * core
    first = (at(r1, p2), at(l1, p2))
    second = (at(p1, r2), at(p1, l2), at(p1, o2))

    barrier = pltpu.get_barrier_semaphore()
    for dev in (partner, *first, *second):
        pl.semaphore_signal(barrier, inc=1, device_id={"tp": dev}, device_id_type=MESH)

    def load(src, dst, sem):
        return pltpu.make_async_copy(src, dst, sem)

    def chunk_loads(c):
        r = pl.ds(pl.multiple_of(c * m, m), m)
        return (
            load(dy.at[r], dyv.at[r], lsem.at[c, 0]),
            load(gate.at[r], gu.at[r, pl.ds(0, f)], lsem.at[c, 1]),
            load(up.at[r], gu.at[r, pl.ds(f, f)], lsem.at[c, 2]),
        )

    def unit_load(j, slot):
        return load(x.at[:, pl.ds(pl.multiple_of(j * uw, uw), uw)], xs.at[slot], xsem.at[slot])

    load_wd = load(wd, wdv, wsem.at[0])
    load_wg = load(wg, wv.at[:, pl.ds(0, f)], wsem.at[1])
    load_wu = load(wu, wv.at[:, pl.ds(f, f)], wsem.at[2])
    first_loads = chunk_loads(0)
    for cp in (first_loads[1], first_loads[2], first_loads[0], load_wd):
        cp.start()

    def send(c, k, src, dst, dev):
        return pltpu.make_async_remote_copy(
            src, dst, ssem.at[c], rsem.at[c, k], device_id={"tp": dev}, device_id_type=MESH
        )

    def place(c, h, piece):
        return pl.ds(pl.multiple_of(c * m + h * half + piece * q, q), q)

    def piece(p):
        return pl.ds(pl.multiple_of(p * q, q), q)

    def cols(p, width):
        return pl.ds(pl.multiple_of(p * width, width), width)

    lo, hi, al = pl.ds(0, ch), pl.ds(ch, ch), pl.ds(0, d)

    def same(c, k, r, w, dev):
        return send(c, k, dx.at[r, w], dx.at[r, w], dev)

    def copy(c, k):
        if k == 0:
            return send(c, 0, sT.at[c], rT.at[c], partner)
        if k <= 2:
            return send(c, k, sA.at[c, k - 1], rA.at[c, k - 1], first[k - 1])
        if k <= 4:
            return send(c, k, sB.at[c, k - 3], rB.at[c, k - 3], first[k - 3])
        if k <= 7:
            return send(c, k, sC.at[c, k - 5], rC.at[c, k - 5], second[k - 5])
        mine = place(c, core, p1)
        if k <= 10:
            return same(c, k, mine, cols(p2, cq), second[k - 8])
        if k <= 12:
            return same(c, k, mine, al, first[k - 11])
        if k == 13:
            return same(c, k, place(c, core, l1), lo, first[0])
        if k == 14:
            return same(c, k, place(c, core, r1), hi, first[1])
        return same(c, k, place(c, core, (p1, l1, r1, o1)[k - 15]), al, partner)

    def arrival(c, k):
        if k <= 7:
            return copy(c, k)
        mine = place(c, core, p1)
        if k <= 10:
            return same(c, k, mine, cols((l2, r2, o2)[k - 8], cq), partner)
        if k <= 12:
            return same(c, k, place(c, core, (l1, r1)[k - 11]), al, partner)
        if k <= 14:
            return same(c, k, place(c, core, o1), (lo, hi)[k - 13], partner)
        s = (p2, l2, r2, o2)[k - 15]
        return same(c, k, place(c, 1 - core, s), al, partner)

    def got(c, *ks):
        for k in ks:
            arrival(c, k).wait_recv()

    def go(c, *ks):
        for k in ks:
            copy(c, k).start()

    def event(k, c):
        acc = own.at[lax.rem(c, SLOTS)]
        if k == 1:
            got(c, 0)
            t = acc[piece(o1), :] + rT[c, piece(o1), :].astype(F32)
            sA[c, 0] = t[:, :ch].astype(BF16)
            sA[c, 1] = t[:, ch:].astype(BF16)
            for p in (r1, l1, p1):
                acc[piece(p), :] = acc[piece(p), :] + rT[c, piece(p), :].astype(F32)
            go(c, 1, 2)
        elif k == 2:
            got(c, 1, 2)
            sB[c, 0, :, lo] = (acc[piece(r1), lo] + rA[c, 0].astype(F32)).astype(BF16)
            sB[c, 0, :, hi] = acc[piece(r1), hi].astype(BF16)
            sB[c, 1, :, lo] = acc[piece(l1), lo].astype(BF16)
            sB[c, 1, :, hi] = (acc[piece(l1), hi] + rA[c, 1].astype(F32)).astype(BF16)
            go(c, 3, 4)
        elif k == 3:
            got(c, 3, 4)
            acc[piece(p1), :] = acc[piece(p1), :] + rB[c, 0].astype(F32) + rB[c, 1].astype(F32)
            for i, p in enumerate((r2, l2, o2)):
                sC[c, i] = acc[piece(p1), cols(p, cq)].astype(BF16)
            fin[c] = acc[piece(p1), cols(p2, cq)]
            go(c, 5, 6, 7)
        elif k == 4:
            got(c, 5, 6, 7)
            t = fin[c] + rC[c, 0].astype(F32) + rC[c, 1].astype(F32) + rC[c, 2].astype(F32)
            dx[place(c, core, p1), cols(p2, cq)] = t.astype(BF16)
            go(c, 8, 9, 10)
        elif k == 5:
            got(c, 8, 9, 10)
            go(c, 11, 12, 15)
        elif k == 6:
            got(c, 11, 12)
            go(c, 13, 14, 16, 17)
        elif k == 7:
            got(c, 13, 14)
            go(c, 18)
        else:
            got(c, 15, 16, 17, 18)

    c0, c1 = math.sqrt(2 / math.pi), math.sqrt(2 / math.pi) * 0.044715

    def hidden_part(c):
        r = pl.ds(pl.multiple_of(c * m, m), m)
        w, w2 = pl.ds(0, f), pl.ds(f, f)
        dh = dot(dyv[r, :], wdv[w, :], 1, 1)
        g = gu[r, w].astype(F32)
        u = gu[r, w2].astype(F32)
        g2 = g * g
        t = jnp.tanh(g * (c0 + c1 * g2))
        hg = 0.5 * g
        s = 1.0 + t
        act = hg * s
        slope = 0.5 * s + hg * (s * (1.0 - t)) * (c0 + (3.0 * c1) * g2)
        hid[r, w] = (act * u).astype(BF16)
        gu[r, w] = (dh * u * slope).astype(BF16)
        gu[r, w2] = (dh * act).astype(BF16)

    def term_part(c):
        base = c * m
        rp = pl.ds(pl.multiple_of(base + (1 - core) * half, half), half)
        ro = pl.ds(pl.multiple_of(base + core * half, half), half)
        lhs = jnp.concatenate([gu[rp, :], gu[ro, :]], 0)
        for k in range(4):
            w = pl.ds(k * cq, cq)
            t = dot(lhs, wv[w, :], 1, 1)
            sT[c, :, w] = t[:half].astype(BF16)
            own[lax.rem(c, SLOTS), :, w] = t[half:]

    def weights_part(j):
        r = pl.ds(pl.multiple_of(j * uw, uw), uw)
        t = dot(xs[lax.rem(j, 2)], gu[...], 0, 0)
        dwg[r, :] = t[:, :f].astype(BF16)
        dwu[r, :] = t[:, f:].astype(BF16)

    def down_part(j):
        w = pl.ds(pl.multiple_of(j * uw, uw), uw)
        dwd[:, w] = dot(hid[...], dyv[:, w], 0, 0).astype(BF16)

    def dx_piece(c, i):
        if i == 0:
            for cp in chunk_loads(c):
                cp.wait()
            hidden_part(c)
        else:
            term_part(c)
            go(c, 0)

            @pl.when(c + 3 < n)
            def _():
                for cp in chunk_loads(c + 3):
                    cp.start()

            @pl.when(c == n - 3)
            def _():
                unit_load(0, 0).start()
                unit_load(1, 1).start()

    def dw_piece(j, i):
        if i == 0:
            unit_load(j, lax.rem(j, 2)).wait()
            weights_part(j)

            @pl.when(j + 2 < units)
            def _():
                unit_load(j + 2, lax.rem(j, 2)).start()
        else:
            down_part(j)

    first_loads[1].wait()
    load_wg.start()
    load_wu.start()
    first_loads[2].wait()
    first_loads[0].wait()
    load_wd.wait()
    hidden_part(0)
    for c in range(1, min(4, n)):
        for cp in chunk_loads(c):
            cp.start()
    load_wg.wait()
    load_wu.wait()
    term_part(0)
    pl.semaphore_wait(barrier, 6)
    go(0, 0)

    def step(t, _):
        for i in range(POINTS):
            @pl.when(t < n)
            def _(i=i):
                dx_piece(t, i)

            @pl.when((t >= n) & (t < n + units))
            def _(i=i):
                dw_piece(t - n, i)

            for k, lag in LAG.items():
                if lag % POINTS == i:
                    c = t - lag // POINTS

                    @pl.when((c >= 0) & (c < n))
                    def _(k=k, c=c):
                        event(k, c)

        return 0

    lax.fori_loop(1, n + max(LAG.values()) // POINTS, step, 0)

    sent = pl.ds(0, half + (2 + 1) * q + 2 * 3 * q // 4 + (2 + 1) * q + 4 * q)
    for c in range(n):
        pltpu.make_async_copy(dx.at[sent], dx.at[sent], ssem.at[c]).wait()


def flush(*refs):
    src, dst, sem = refs[:4], refs[4:8], refs[8]
    copies, cuts = [], (8, 2, 2, 2)
    for a, b, cut in zip(src, dst, cuts):
        size = a.shape[0] // cut
        for i in range(cut):
            r = pl.ds(i * size, size)
            copies.append(pltpu.make_async_copy(a.at[r], b.at[r], sem.at[len(copies)]))
    for cp in copies:
        cp.start()
    for cp in copies:
        cp.wait()


def solution(mesh):
    side = math.isqrt(mesh.shape["tp"] // 2)

    def step(x, dy, gate, up, w_gate, w_up, w_down):
        (rows, d), f = x.shape, gate.shape[1]
        m = min(CHUNK, rows)
        n, half, q = rows // m, m // 2, m // 8
        vm = pltpu.VMEM
        results = pl.pallas_call(
            functools.partial(kernel, side),
            out_shape=[vm((rows, d), BF16), vm((d, f), BF16), vm((d, f), BF16), vm((f, d), BF16)],
            in_specs=[pl.BlockSpec(memory_space=pl.ANY)] * 7,
            out_specs=[pl.BlockSpec(memory_space=pltpu.VMEM)] * 4,
            scratch_shapes=[
                vm((f, d), BF16), vm((d, 2 * f), BF16), vm((rows, d), BF16), vm((rows, 2 * f), BF16), vm((rows, f), BF16),
                vm((2, rows, d // n), BF16), vm((SLOTS, half, d), F32), vm((n, q, d // 4), F32),
                vm((n, half, d), BF16), vm((n, half, d), BF16),
                vm((n, 2, q, d // 2), BF16), vm((n, 2, q, d // 2), BF16),
                vm((n, 2, q, d), BF16), vm((n, 2, q, d), BF16),
                vm((n, 3, q, d // 4), BF16), vm((n, 3, q, d // 4), BF16),
                pltpu.SemaphoreType.DMA((3,)), pltpu.SemaphoreType.DMA((n, 3)), pltpu.SemaphoreType.DMA((2,)),
                pltpu.SemaphoreType.DMA((n,)), pltpu.SemaphoreType.DMA((n, COPIES)),
            ],
            compiler_params=pltpu.CompilerParams(
                collective_id=0, has_side_effects=True, vmem_limit_bytes=49 * 2**20 + 2**19
            ),
        )(x, dy, gate, up, w_gate, w_up, w_down)
        return tuple(pl.pallas_call(
            flush,
            out_shape=[jax.ShapeDtypeStruct(a.shape, a.dtype) for a in results],
            in_specs=[pl.BlockSpec(memory_space=pltpu.VMEM)] * 4,
            out_specs=[pl.BlockSpec(memory_space=pl.ANY)] * 4,
            scratch_shapes=[pltpu.SemaphoreType.DMA((14,))],
            compiler_params=pltpu.CompilerParams(vmem_limit_bytes=2**20),
        )(*results))

    tokens, columns, by_rows = P("dp", None), P(None, "tp"), P("tp", None)
    return jax.shard_map(
        step,
        mesh=mesh,
        in_specs=(tokens, tokens, P("dp", "tp"), P("dp", "tp"), columns, columns, by_rows),
        out_specs=(tokens, P("dp", "tp"), P("dp", "tp"), P(("dp", "tp"), None)),
        check_vma=False,
    )
```

```python
import functools
import math

import jax
import jax.numpy as jnp
from jax import lax
from jax.experimental import pallas as pl
from jax.experimental.pallas import tpu as pltpu
from jax.sharding import PartitionSpec as P

MESH = pl.DeviceIdType.MESH
CHUNK = 256
PARTS = 2
BF16, F32 = jnp.bfloat16, jnp.float32
EVENT = (0, 1, 1, 2, 2, 3, 3, 3, 4, 4, 4, 5, 5, 6, 6, 7, 7, 7, 7)
SLOTS = 12
POINTS = 2
LAG = {1: 2, 2: 5, 3: 9, 4: 14, 5: 19, 6: 30, 7: 47, 8: 63}


def dot(a, b, ca, cb):
    return lax.dot_general(a, b, (((ca,), (cb,)), ((), ())), preferred_element_type=F32)


def kernel(side, x, dy, gate, up, wg, wu, wd, dx, dwg, dwu, dwd,
           wdv, wv, dyv, gu, hid, xs, own, fin, sT, rT, sA, rA, sB, rB, sC, rC, wsem, lsem, xsem, ssem, rsem):
    rows, d = dx.shape
    f = wd.shape[0]
    m = min(CHUNK, rows)
    n = rows // m
    mp, parts = m // PARTS, n * PARTS
    half, q = mp // 2, mp // 8
    ch, cq = d // 2, d // 4
    units, uw = n, d // n

    me = lax.axis_index("tp")
    core = lax.rem(me, 2)
    chip = me // 2
    px, py = chip // side, lax.rem(chip, side)
    p1 = px + core * (py - px)
    p2 = py + core * (px - py)

    def at(a, b):
        return ((1 - core) * (a * side + b) + core * (b * side + a)) * 2 + core

    def turn(p, k):
        return lax.rem(p + k, side)

    r1, o1, l1 = turn(p1, 1), turn(p1, 2), turn(p1, 3)
    r2, o2, l2 = turn(p2, 1), turn(p2, 2), turn(p2, 3)
    partner = me + 1 - 2 * core
    first = (at(r1, p2), at(l1, p2))
    second = (at(p1, r2), at(p1, l2), at(p1, o2))

    barrier = pltpu.get_barrier_semaphore()
    for dev in (partner, *first, *second):
        pl.semaphore_signal(barrier, inc=1, device_id={"tp": dev}, device_id_type=MESH)

    def load(src, dst, sem):
        return pltpu.make_async_copy(src, dst, sem)

    def chunk_loads(c):
        r = pl.ds(pl.multiple_of(c * m, m), m)
        return (
            load(dy.at[r], dyv.at[r], lsem.at[c, 0]),
            load(gate.at[r], gu.at[r, pl.ds(0, f)], lsem.at[c, 1]),
            load(up.at[r], gu.at[r, pl.ds(f, f)], lsem.at[c, 2]),
        )

    def unit_load(j, slot):
        return load(x.at[:, pl.ds(pl.multiple_of(j * uw, uw), uw)], xs.at[slot], xsem.at[slot])

    load_wd = load(wd, wdv, wsem.at[0])
    load_wg = load(wg, wv.at[:, pl.ds(0, f)], wsem.at[1])
    load_wu = load(wu, wv.at[:, pl.ds(f, f)], wsem.at[2])
    first_loads = chunk_loads(0)
    for cp in (first_loads[1], first_loads[2], first_loads[0], load_wd):
        cp.start()

    def send(c, k, src, dst, dev):
        return pltpu.make_async_remote_copy(
            src, dst, ssem.at[c], rsem.at[c, EVENT[k]], device_id={"tp": dev}, device_id_type=MESH
        )

    def place(c, h, piece):
        return pl.ds(pl.multiple_of(c * mp + h * half + piece * q, q), q)

    def piece(p):
        return pl.ds(pl.multiple_of(p * q, q), q)

    def cols(p, width):
        return pl.ds(pl.multiple_of(p * width, width), width)

    lo, hi, al = pl.ds(0, ch), pl.ds(ch, ch), pl.ds(0, d)

    def same(c, k, r, w, dev):
        return send(c, k, dx.at[r, w], dx.at[r, w], dev)

    def copy(c, k):
        if k == 0:
            return send(c, 0, sT.at[c], rT.at[c], partner)
        if k <= 2:
            return send(c, k, sA.at[c, k - 1], rA.at[c, k - 1], first[k - 1])
        if k <= 4:
            return send(c, k, sB.at[c, k - 3], rB.at[c, k - 3], first[k - 3])
        if k <= 7:
            return send(c, k, sC.at[c, k - 5], rC.at[c, k - 5], second[k - 5])
        mine = place(c, core, p1)
        if k <= 10:
            return same(c, k, mine, cols(p2, cq), second[k - 8])
        if k <= 12:
            return same(c, k, mine, al, first[k - 11])
        if k == 13:
            return same(c, k, place(c, core, l1), lo, first[0])
        if k == 14:
            return same(c, k, place(c, core, r1), hi, first[1])
        return same(c, k, place(c, core, (p1, l1, r1, o1)[k - 15]), al, partner)

    arriving = ((half, d), (q, d), (2 * q, d), (q, 3 * cq), (q, 3 * cq), (2 * q, d), (q, d), (4 * q, d))

    def got(c, k):
        r, w = arriving[k - 1]
        some = dx.at[pl.ds(0, r), pl.ds(0, w)]
        pltpu.make_async_copy(some, some, rsem.at[c, k - 1]).wait()

    def go(c, *ks):
        for k in ks:
            copy(c, k).start()

    def event(k, c):
        acc = own.at[lax.rem(c, SLOTS)]
        if k == 1:
            got(c, k)
            t = acc[piece(o1), :] + rT[c, piece(o1), :].astype(F32)
            sA[c, 0] = t[:, :ch].astype(BF16)
            sA[c, 1] = t[:, ch:].astype(BF16)
            for p in (r1, l1, p1):
                acc[piece(p), :] = acc[piece(p), :] + rT[c, piece(p), :].astype(F32)
            go(c, 1, 2)
        elif k == 2:
            got(c, k)
            sB[c, 0, :, lo] = (acc[piece(r1), lo] + rA[c, 0].astype(F32)).astype(BF16)
            sB[c, 0, :, hi] = acc[piece(r1), hi].astype(BF16)
            sB[c, 1, :, lo] = acc[piece(l1), lo].astype(BF16)
            sB[c, 1, :, hi] = (acc[piece(l1), hi] + rA[c, 1].astype(F32)).astype(BF16)
            go(c, 3, 4)
        elif k == 3:
            got(c, k)
            acc[piece(p1), :] = acc[piece(p1), :] + rB[c, 0].astype(F32) + rB[c, 1].astype(F32)
            for i, p in enumerate((r2, l2, o2)):
                sC[c, i] = acc[piece(p1), cols(p, cq)].astype(BF16)
            fin[c] = acc[piece(p1), cols(p2, cq)]
            go(c, 5, 6, 7)
        elif k == 4:
            got(c, k)
            t = fin[c] + rC[c, 0].astype(F32) + rC[c, 1].astype(F32) + rC[c, 2].astype(F32)
            dx[place(c, core, p1), cols(p2, cq)] = t.astype(BF16)
            go(c, 8, 9, 10)
        elif k == 5:
            got(c, k)
            go(c, 11, 12, 15)
        elif k == 6:
            got(c, k)
            go(c, 13, 14, 16, 17)
        elif k == 7:
            got(c, k)
            go(c, 18)
        else:
            got(c, k)

    c0, c1 = math.sqrt(2 / math.pi), math.sqrt(2 / math.pi) * 0.044715

    def hidden_part(c):
        r = pl.ds(pl.multiple_of(c * m, m), m)
        w, w2 = pl.ds(0, f), pl.ds(f, f)
        dh = dot(dyv[r, :], wdv[w, :], 1, 1)
        g = gu[r, w].astype(F32)
        u = gu[r, w2].astype(F32)
        g2 = g * g
        t = jnp.tanh(g * (c0 + c1 * g2))
        hg = 0.5 * g
        s = 1.0 + t
        act = hg * s
        slope = 0.5 * s + hg * (s * (1.0 - t)) * (c0 + (3.0 * c1) * g2)
        hid[r, w] = (act * u).astype(BF16)
        gu[r, w] = (dh * u * slope).astype(BF16)
        gu[r, w2] = (dh * act).astype(BF16)

    def term_part(c):
        def rows_of(s, h):
            return gu[pl.ds(pl.multiple_of(c * m + s * mp + h * half, half), half), :]

        lhs = jnp.concatenate(
            [rows_of(s, 1 - core) for s in range(PARTS)] + [rows_of(s, core) for s in range(PARTS)], 0
        )
        for k in range(4):
            w = pl.ds(k * cq, cq)
            t = dot(lhs, wv[w, :], 1, 1)
            for s in range(PARTS):
                p = c * PARTS + s
                sT[p, :, w] = t[s * half : (s + 1) * half].astype(BF16)
                own[lax.rem(p, SLOTS), :, w] = t[(PARTS + s) * half : (PARTS + s + 1) * half]

    def send_term(c):
        for s in range(PARTS):
            go(c * PARTS + s, 0)

    def weights_part(j):
        r = pl.ds(pl.multiple_of(j * uw, uw), uw)
        t = dot(xs[lax.rem(j, 2)], gu[...], 0, 0)
        dwg[r, :] = t[:, :f].astype(BF16)
        dwu[r, :] = t[:, f:].astype(BF16)

    def down_part(j):
        w = pl.ds(pl.multiple_of(j * uw, uw), uw)
        dwd[:, w] = dot(hid[...], dyv[:, w], 0, 0).astype(BF16)

    def dx_piece(c, i):
        if i == 0:
            for cp in chunk_loads(c):
                cp.wait()
            hidden_part(c)
        else:
            term_part(c)
            send_term(c)

            @pl.when(c + 3 < n)
            def _():
                for cp in chunk_loads(c + 3):
                    cp.start()

            @pl.when(c == n - 3)
            def _():
                unit_load(0, 0).start()
                unit_load(1, 1).start()

    def dw_piece(j, i):
        if i == 0:
            unit_load(j, lax.rem(j, 2)).wait()
            weights_part(j)

            @pl.when(j + 2 < units)
            def _():
                unit_load(j + 2, lax.rem(j, 2)).start()
        else:
            down_part(j)

    first_loads[1].wait()
    load_wg.start()
    load_wu.start()
    first_loads[2].wait()
    first_loads[0].wait()
    load_wd.wait()
    hidden_part(0)
    for c in range(1, min(4, n)):
        for cp in chunk_loads(c):
            cp.start()
    load_wg.wait()
    load_wu.wait()
    term_part(0)
    pl.semaphore_wait(barrier, 6)
    send_term(0)

    def step(t, _):
        for i in range(POINTS):
            @pl.when(t < n)
            def _(i=i):
                dx_piece(t, i)

            @pl.when((t >= n) & (t < n + units))
            def _(i=i):
                dw_piece(t - n, i)

            for k, lag in LAG.items():
                for s in range(PARTS):
                    if (lag + s) % POINTS == i:
                        c = t - (lag + s) // POINTS

                        @pl.when((c >= 0) & (c < n))
                        def _(k=k, c=c, s=s):
                            event(k, c * PARTS + s)

        return 0

    lax.fori_loop(1, n + (max(LAG.values()) + PARTS - 1) // POINTS, step, 0)

    sent = pl.ds(0, sum(r * w for r, w in arriving) // d)
    for c in range(parts):
        pltpu.make_async_copy(dx.at[sent], dx.at[sent], ssem.at[c]).wait()


def flush(*refs):
    src, dst, sem = refs[:4], refs[4:8], refs[8]
    copies, cuts = [], (8, 2, 2, 2)
    for a, b, cut in zip(src, dst, cuts):
        size = a.shape[0] // cut
        for i in range(cut):
            r = pl.ds(i * size, size)
            copies.append(pltpu.make_async_copy(a.at[r], b.at[r], sem.at[len(copies)]))
    for cp in copies:
        cp.start()
    for cp in copies:
        cp.wait()


def solution(mesh):
    side = math.isqrt(mesh.shape["tp"] // 2)

    def step(x, dy, gate, up, w_gate, w_up, w_down):
        (rows, d), f = x.shape, gate.shape[1]
        m = min(CHUNK, rows)
        n, mp = rows // m, m // PARTS
        parts, half, q = n * PARTS, mp // 2, mp // 8
        vm = pltpu.VMEM
        results = pl.pallas_call(
            functools.partial(kernel, side),
            out_shape=[vm((rows, d), BF16), vm((d, f), BF16), vm((d, f), BF16), vm((f, d), BF16)],
            in_specs=[pl.BlockSpec(memory_space=pl.ANY)] * 7,
            out_specs=[pl.BlockSpec(memory_space=pltpu.VMEM)] * 4,
            scratch_shapes=[
                vm((f, d), BF16), vm((d, 2 * f), BF16), vm((rows, d), BF16), vm((rows, 2 * f), BF16), vm((rows, f), BF16),
                vm((2, rows, d // n), BF16), vm((SLOTS, half, d), F32), vm((parts, q, d // 4), F32),
                vm((parts, half, d), BF16), vm((parts, half, d), BF16),
                vm((parts, 2, q, d // 2), BF16), vm((parts, 2, q, d // 2), BF16),
                vm((parts, 2, q, d), BF16), vm((parts, 2, q, d), BF16),
                vm((parts, 3, q, d // 4), BF16), vm((parts, 3, q, d // 4), BF16),
                pltpu.SemaphoreType.DMA((3,)), pltpu.SemaphoreType.DMA((n, 3)), pltpu.SemaphoreType.DMA((2,)),
                pltpu.SemaphoreType.DMA((parts,)), pltpu.SemaphoreType.DMA((parts, 8)),
            ],
            compiler_params=pltpu.CompilerParams(
                collective_id=0, has_side_effects=True, vmem_limit_bytes=49 * 2**20 + 2**19
            ),
        )(x, dy, gate, up, w_gate, w_up, w_down)
        return tuple(pl.pallas_call(
            flush,
            out_shape=[jax.ShapeDtypeStruct(a.shape, a.dtype) for a in results],
            in_specs=[pl.BlockSpec(memory_space=pltpu.VMEM)] * 4,
            out_specs=[pl.BlockSpec(memory_space=pl.ANY)] * 4,
            scratch_shapes=[pltpu.SemaphoreType.DMA((14,))],
            compiler_params=pltpu.CompilerParams(vmem_limit_bytes=2**20),
        )(*results))

    tokens, columns, by_rows = P("dp", None), P(None, "tp"), P("tp", None)
    return jax.shard_map(
        step,
        mesh=mesh,
        in_specs=(tokens, tokens, P("dp", "tp"), P("dp", "tp"), columns, columns, by_rows),
        out_specs=(tokens, P("dp", "tp"), P("dp", "tp"), P(("dp", "tp"), None)),
        check_vma=False,
    )
```

```python
import functools
import math

import jax
import jax.numpy as jnp
from jax import lax
from jax.experimental import pallas as pl
from jax.experimental.pallas import tpu as pltpu
from jax.sharding import PartitionSpec as P

MESH = pl.DeviceIdType.MESH
CHUNK = 256
PARTS = 2
BF16, F32 = jnp.bfloat16, jnp.float32
EVENT = (0, 1, 1, 2, 2, 3, 3, 3, 4, 4, 4, 5, 5, 6, 6, 7, 7, 7, 7)
SLOTS = 12
POINTS = 2
LAG = {1: 2, 2: 5, 3: 9, 4: 14, 5: 19, 6: 30, 7: 47}


def dot(a, b, ca, cb):
    return lax.dot_general(a, b, (((ca,), (cb,)), ((), ())), preferred_element_type=F32)


def kernel(side, x, dy, gate, up, wg, wu, wd, dx, dwg, dwu, dwd,
           wdv, wv, dyv, gu, hid, xs, own, fin, sT, rT, sA, rA, sB, rB, sC, rC, wsem, lsem, xsem, ssem, rsem, psem):
    rows, d = dx.shape
    f = wd.shape[0]
    m = min(CHUNK, rows)
    n = rows // m
    mp, parts = m // PARTS, n * PARTS
    half, q = mp // 2, mp // 8
    ch, cq = d // 2, d // 4
    units, uw = n, d // n

    me = lax.axis_index("tp")
    core = lax.rem(me, 2)
    chip = me // 2
    px, py = chip // side, lax.rem(chip, side)
    p1 = px + core * (py - px)
    p2 = py + core * (px - py)

    def at(a, b):
        return ((1 - core) * (a * side + b) + core * (b * side + a)) * 2 + core

    def turn(p, k):
        return lax.rem(p + k, side)

    r1, o1, l1 = turn(p1, 1), turn(p1, 2), turn(p1, 3)
    r2, o2, l2 = turn(p2, 1), turn(p2, 2), turn(p2, 3)
    partner = me + 1 - 2 * core
    first = (at(r1, p2), at(l1, p2))
    second = (at(p1, r2), at(p1, l2), at(p1, o2))

    barrier = pltpu.get_barrier_semaphore()
    for dev in (partner, *first, *second):
        pl.semaphore_signal(barrier, inc=1, device_id={"tp": dev}, device_id_type=MESH)

    def load(src, dst, sem):
        return pltpu.make_async_copy(src, dst, sem)

    def chunk_loads(c):
        r = pl.ds(pl.multiple_of(c * m, m), m)
        return (
            load(dy.at[r], dyv.at[r], lsem.at[lax.rem(c, 4), 0]),
            load(gate.at[r], gu.at[r, pl.ds(0, f)], lsem.at[lax.rem(c, 4), 1]),
            load(up.at[r], gu.at[r, pl.ds(f, f)], lsem.at[lax.rem(c, 4), 2]),
        )

    def unit_load(j, slot):
        return load(x.at[:, pl.ds(pl.multiple_of(j * uw, uw), uw)], xs.at[slot], xsem.at[slot])

    load_wd = load(wd, wdv, wsem.at[0])
    load_wg = load(wg, wv.at[:, pl.ds(0, f)], wsem.at[1])
    load_wu = load(wu, wv.at[:, pl.ds(f, f)], wsem.at[2])
    first_loads = chunk_loads(0)
    for cp in (first_loads[1], first_loads[2], first_loads[0], load_wd):
        cp.start()

    def send(c, k, src, dst, dev):
        arrived = rsem.at[c, EVENT[k]] if EVENT[k] < 7 else psem.at[0]
        return pltpu.make_async_remote_copy(
            src, dst, ssem.at[lax.div(c, parts // 2)], arrived, device_id={"tp": dev}, device_id_type=MESH
        )

    def place(c, h, piece):
        return pl.ds(pl.multiple_of(c * mp + h * half + piece * q, q), q)

    def piece(p):
        return pl.ds(pl.multiple_of(p * q, q), q)

    def cols(p, width):
        return pl.ds(pl.multiple_of(p * width, width), width)

    lo, hi, al = pl.ds(0, ch), pl.ds(ch, ch), pl.ds(0, d)

    def same(c, k, r, w, dev):
        return send(c, k, dx.at[r, w], dx.at[r, w], dev)

    def copy(c, k):
        if k == 0:
            return send(c, 0, sT.at[c], rT.at[c], partner)
        if k <= 2:
            return send(c, k, sA.at[c, k - 1], rA.at[c, k - 1], first[k - 1])
        if k <= 4:
            return send(c, k, sB.at[c, k - 3], rB.at[c, k - 3], first[k - 3])
        if k <= 7:
            return send(c, k, sC.at[c, k - 5], rC.at[c, k - 5], second[k - 5])
        mine = place(c, core, p1)
        if k <= 10:
            return same(c, k, mine, cols(p2, cq), second[k - 8])
        if k <= 12:
            return same(c, k, mine, al, first[k - 11])
        if k == 13:
            return same(c, k, place(c, core, l1), lo, first[0])
        if k == 14:
            return same(c, k, place(c, core, r1), hi, first[1])
        return same(c, k, place(c, core, (p1, l1, r1, o1)[k - 15]), al, partner)

    arriving = ((half, d), (q, d), (2 * q, d), (q, 3 * cq), (q, 3 * cq), (2 * q, d), (q, d), (4 * q, d))

    def take(sem, r, w):
        some = dx.at[pl.ds(0, r), pl.ds(0, w)]
        pltpu.make_async_copy(some, some, sem).wait()

    def got(c, k):
        r, w = arriving[k - 1]
        take(rsem.at[c, k - 1], r, w)

    def go(c, *ks):
        for k in ks:
            copy(c, k).start()

    def event(k, c):
        acc = own.at[lax.rem(c, SLOTS)]
        if k == 1:
            t = acc[piece(o1), :] + rT[c, piece(o1), :].astype(F32)
            sA[c, 0] = t[:, :ch].astype(BF16)
            sA[c, 1] = t[:, ch:].astype(BF16)
            for p in (r1, l1, p1):
                acc[piece(p), :] = acc[piece(p), :] + rT[c, piece(p), :].astype(F32)
            go(c, 1, 2)
        elif k == 2:
            sB[c, 0, :, lo] = (acc[piece(r1), lo] + rA[c, 0].astype(F32)).astype(BF16)
            sB[c, 0, :, hi] = acc[piece(r1), hi].astype(BF16)
            sB[c, 1, :, lo] = acc[piece(l1), lo].astype(BF16)
            sB[c, 1, :, hi] = (acc[piece(l1), hi] + rA[c, 1].astype(F32)).astype(BF16)
            go(c, 3, 4)
        elif k == 3:
            acc[piece(p1), :] = acc[piece(p1), :] + rB[c, 0].astype(F32) + rB[c, 1].astype(F32)
            for i, p in enumerate((r2, l2, o2)):
                sC[c, i] = acc[piece(p1), cols(p, cq)].astype(BF16)
            fin[c] = acc[piece(p1), cols(p2, cq)]
            go(c, 5, 6, 7)
        elif k == 4:
            t = fin[c] + rC[c, 0].astype(F32) + rC[c, 1].astype(F32) + rC[c, 2].astype(F32)
            dx[place(c, core, p1), cols(p2, cq)] = t.astype(BF16)
            go(c, 8, 9, 10)
        elif k == 5:
            go(c, 11, 12, 15)
        elif k == 6:
            go(c, 13, 14, 16, 17)
        else:
            go(c, 18)

    c0, c1 = math.sqrt(2 / math.pi), math.sqrt(2 / math.pi) * 0.044715

    def hidden_part(c):
        r = pl.ds(pl.multiple_of(c * m, m), m)
        w, w2 = pl.ds(0, f), pl.ds(f, f)
        dh = dot(dyv[r, :], wdv[w, :], 1, 1)
        g = gu[r, w].astype(F32)
        u = gu[r, w2].astype(F32)
        g2 = g * g
        t = jnp.tanh(g * (c0 + c1 * g2))
        hg = 0.5 * g
        s = 1.0 + t
        act = hg * s
        slope = 0.5 * s + hg * (s * (1.0 - t)) * (c0 + (3.0 * c1) * g2)
        hid[r, w] = (act * u).astype(BF16)
        gu[r, w] = (dh * u * slope).astype(BF16)
        gu[r, w2] = (dh * act).astype(BF16)

    def term_part(c):
        def rows_of(s, h):
            return gu[pl.ds(pl.multiple_of(c * m + s * mp + h * half, half), half), :]

        lhs = jnp.concatenate(
            [rows_of(s, 1 - core) for s in range(PARTS)] + [rows_of(s, core) for s in range(PARTS)], 0
        )
        for k in range(4):
            w = pl.ds(k * cq, cq)
            t = dot(lhs, wv[w, :], 1, 1)
            for s in range(PARTS):
                p = c * PARTS + s
                sT[p, :, w] = t[s * half : (s + 1) * half].astype(BF16)
                own[lax.rem(p, SLOTS), :, w] = t[(PARTS + s) * half : (PARTS + s + 1) * half]

    def send_term(c):
        for s in range(PARTS):
            go(c * PARTS + s, 0)

    def weights_part(j):
        r = pl.ds(pl.multiple_of(j * uw, uw), uw)
        t = dot(xs[lax.rem(j, 2)], gu[...], 0, 0)
        dwg[r, :] = t[:, :f].astype(BF16)
        dwu[r, :] = t[:, f:].astype(BF16)

    def down_part(j):
        w = pl.ds(pl.multiple_of(j * uw, uw), uw)
        dwd[:, w] = dot(hid[...], dyv[:, w], 0, 0).astype(BF16)

    def dx_piece(c, i):
        if i == 0:
            for cp in chunk_loads(c):
                cp.wait()
            hidden_part(c)
        else:
            term_part(c)
            send_term(c)

            @pl.when(c + 3 < n)
            def _():
                for cp in chunk_loads(c + 3):
                    cp.start()

            @pl.when(c == n - 3)
            def _():
                unit_load(0, 0).start()
                unit_load(1, 1).start()

    def dw_piece(j, i):
        if i == 0:
            unit_load(j, lax.rem(j, 2)).wait()
            weights_part(j)

            @pl.when(j + 2 < units)
            def _():
                unit_load(j + 2, lax.rem(j, 2)).start()
        else:
            down_part(j)

    first_loads[1].wait()
    load_wg.start()
    load_wu.start()
    first_loads[2].wait()
    first_loads[0].wait()
    load_wd.wait()
    hidden_part(0)
    for c in range(1, min(4, n)):
        for cp in chunk_loads(c):
            cp.start()
    load_wg.wait()
    load_wu.wait()
    term_part(0)
    pl.semaphore_wait(barrier, 6)
    send_term(0)

    def step(t, _):
        for i in range(POINTS):
            @pl.when(t < n)
            def _(i=i):
                dx_piece(t, i)

            @pl.when((t >= n) & (t < n + units))
            def _(i=i):
                dw_piece(t - n, i)

            for k, lag in LAG.items():
                for s in range(PARTS):
                    if (lag + s) % POINTS == i:
                        c = t - (lag + s) // POINTS

                        @pl.when((c >= 0) & (c < n))
                        def _(k=k, c=c, s=s):
                            got(c * PARTS + s, k)
                            event(k, c * PARTS + s)

        return 0

    lax.fori_loop(1, n + (max(LAG.values()) + PARTS - 1) // POINTS, step, 0)

    take(psem.at[0], parts * arriving[7][0], d)
    for i in range(2):
        take(ssem.at[i], parts // 2 * sum(r * w for r, w in arriving) // d, d)


def flush(*refs):
    src, dst, sem = refs[:4], refs[4:8], refs[8]
    copies, cuts = [], (8, 2, 2, 2)
    for a, b, cut in zip(src, dst, cuts):
        size = a.shape[0] // cut
        for i in range(cut):
            r = pl.ds(i * size, size)
            copies.append(pltpu.make_async_copy(a.at[r], b.at[r], sem.at[len(copies)]))
    for cp in copies:
        cp.start()
    for cp in copies:
        cp.wait()


def solution(mesh):
    side = math.isqrt(mesh.shape["tp"] // 2)

    def step(x, dy, gate, up, w_gate, w_up, w_down):
        (rows, d), f = x.shape, gate.shape[1]
        m = min(CHUNK, rows)
        n, mp = rows // m, m // PARTS
        parts, half, q = n * PARTS, mp // 2, mp // 8
        vm = pltpu.VMEM
        results = pl.pallas_call(
            functools.partial(kernel, side),
            out_shape=[vm((rows, d), BF16), vm((d, f), BF16), vm((d, f), BF16), vm((f, d), BF16)],
            in_specs=[pl.BlockSpec(memory_space=pl.ANY)] * 7,
            out_specs=[pl.BlockSpec(memory_space=pltpu.VMEM)] * 4,
            scratch_shapes=[
                vm((f, d), BF16), vm((d, 2 * f), BF16), vm((rows, d), BF16), vm((rows, 2 * f), BF16), vm((rows, f), BF16),
                vm((2, rows, d // n), BF16), vm((SLOTS, half, d), F32), vm((parts, q, d // 4), F32),
                vm((parts, half, d), BF16), vm((parts, half, d), BF16),
                vm((parts, 2, q, d // 2), BF16), vm((parts, 2, q, d // 2), BF16),
                vm((parts, 2, q, d), BF16), vm((parts, 2, q, d), BF16),
                vm((parts, 3, q, d // 4), BF16), vm((parts, 3, q, d // 4), BF16),
                pltpu.SemaphoreType.DMA((3,)), pltpu.SemaphoreType.DMA((4, 3)), pltpu.SemaphoreType.DMA((2,)),
                pltpu.SemaphoreType.DMA((2,)), pltpu.SemaphoreType.DMA((parts, 7)), pltpu.SemaphoreType.DMA((1,)),
            ],
            compiler_params=pltpu.CompilerParams(
                collective_id=0, has_side_effects=True, vmem_limit_bytes=49 * 2**20 + 2**19
            ),
        )(x, dy, gate, up, w_gate, w_up, w_down)
        return tuple(pl.pallas_call(
            flush,
            out_shape=[jax.ShapeDtypeStruct(a.shape, a.dtype) for a in results],
            in_specs=[pl.BlockSpec(memory_space=pltpu.VMEM)] * 4,
            out_specs=[pl.BlockSpec(memory_space=pl.ANY)] * 4,
            scratch_shapes=[pltpu.SemaphoreType.DMA((14,))],
            compiler_params=pltpu.CompilerParams(vmem_limit_bytes=2**20),
        )(*results))

    tokens, columns, by_rows = P("dp", None), P(None, "tp"), P("tp", None)
    return jax.shard_map(
        step,
        mesh=mesh,
        in_specs=(tokens, tokens, P("dp", "tp"), P("dp", "tp"), columns, columns, by_rows),
        out_specs=(tokens, P("dp", "tp"), P("dp", "tp"), P(("dp", "tp"), None)),
        check_vma=False,
    )
```
